128 devices in a mesh: lat: 8 (over y, z_lo), lon: 16 (over x, z_hi, core).
Axes of the slice: x: 4, y: 4, z: 4 (z_hi: 2, z_lo: 2; z = z_hi * 2 + z_lo), core: 2. Of those that a mesh axis runs over, the one named last changes fastest.
Arguments:
- x_first: bfloat16 [4, 48, 192, 512], P(None, 'lat', 'lon'), may hold values from -6 to 6
- x_second: bfloat16 [4, 48, 192, 512], P(None, 'lat', 'lon'), may hold values from -6 to 6
- cotangent: bfloat16 [4, 48, 192, 512], P(None, 'lat', 'lon'), may hold values from -6 to 6
- w_attn_in: bfloat16 [2, 512, 1536], replicated, may hold values from -0.25 to 0.25
- w_attn_out: bfloat16 [2, 512, 512], replicated, may hold values from -0.25 to 0.25
- w_up: bfloat16 [2, 512, 2048], replicated, may hold values from -0.25 to 0.25
- w_down: bfloat16 [2, 2048, 512], replicated, may hold values from -0.125 to 0.125
- norm_gains: float32 [2, 2, 512], replicated, may hold values from 0.1 to 1.9
- logit_scales: float32 [2, 8], replicated, may hold values from 2 to 30
Outputs:
- grad_first: float32 [4, 48, 192, 512], P(None, 'lat', 'lon')
- grad_second: float32 [4, 48, 192, 512], P(None, 'lat', 'lon')
The draws below stay inside these ranges and needn't reach their ends.
All inputs are finite; a program needn't handle non-finite values.
Results may differ from the reference program's by a relative error of at most 0.022.
Values may be sent and summed in bfloat16 or wider, within the bound.
A program may use at most 192 MiB of HBM per device.

```python
import math
import jax
import jax.numpy as jnp
from jax import lax

D = 512
FF = 2048
HEADS = 8
LEVELS = 4
WIN_LEV = 2
WIN_LAT = 6
WIN_LON = 12
NLAT = 48
NLON = 192


def shard_levels(own_key, extent, cuts, smallest, largest):
    factor_of = 1.0
    for position, parts in cuts:
        draws = jax.random.uniform(jax.random.fold_in(jax.random.fold_in(own_key, 6), position), (parts,), jnp.float32, smallest / len(cuts), largest / len(cuts))
        factor_of = factor_of * jnp.repeat(jnp.exp(draws), extent[position] // parts).reshape((-1,) + (1,) * (len(extent) - 1 - position))
    return factor_of


def centred(stream_key, dims, width, most, split=(), kind=jnp.bfloat16):
    drawn = width * jax.random.normal(stream_key, dims, jnp.float32)
    if split:
        drawn = drawn * shard_levels(stream_key, dims, split, -0.22, 0.18)
    return jnp.clip(drawn, -most, most).astype(kind)


def setup_inputs(seed: int = 0) -> dict:
    key_list = jax.random.split(jax.random.key(seed), 10)
    x_first = centred(key_list[0], (LEVELS, NLAT, NLON, D), 1.0, 6.0, ((1, 8), (2, 16)))
    x_second = centred(key_list[1], (LEVELS, NLAT, NLON, D), 1.0, 6.0, ((1, 8), (2, 16)))
    cotangent = centred(key_list[2], (LEVELS, NLAT, NLON, D), 1.0, 6.0, ((1, 8), (2, 16)))
    w_attn_in = centred(key_list[3], (2, D, 3 * D), D ** -0.5, 0.25)
    w_attn_out = centred(key_list[4], (2, D, D), D ** -0.5, 0.25)
    w_up = centred(key_list[5], (2, D, FF), D ** -0.5, 0.25)
    w_down = centred(key_list[6], (2, FF, D), FF ** -0.5, 0.125)
    norm_gains = jnp.clip(1.0 + 0.18 * jax.random.normal(key_list[7], (2, 2, D), jnp.float32), 0.1, 1.9)
    logit_scales = jnp.clip(jnp.exp(jax.random.uniform(key_list[8], (2, HEADS), jnp.float32, math.log(2.0), math.log(30.0))), 2.0, 30.0)
    return {"x_first": x_first, "x_second": x_second, "cotangent": cotangent, "w_attn_in": w_attn_in, "w_attn_out": w_attn_out, "w_up": w_up, "w_down": w_down, "norm_gains": norm_gains, "logit_scales": logit_scales}


EPSILON = 1e-05

def layer_norm(tokens_in, gain_vector):
    center = tokens_in - lax.optimization_barrier(jnp.mean(tokens_in, axis=-1, keepdims=True))
    spread = lax.optimization_barrier(jnp.mean(center * center, axis=-1, keepdims=True))
    return center * lax.rsqrt(spread + EPSILON) * gain_vector

def unit_rows(vectors):
    return vectors * lax.rsqrt(lax.optimization_barrier(jnp.sum(vectors * vectors, axis=-1, keepdims=True)) + 1e-06)

def swin_block(windows, labels, w_in, w_out, w_upper, w_lower, gains, scales):
    window_count, length, feature_width = windows.shape
    head_count = scales.shape[0]
    head_size = feature_width // head_count
    normed = layer_norm(windows, gains[0]).astype(jnp.bfloat16)
    projected = jnp.dot(normed.reshape(window_count * length, feature_width), w_in, preferred_element_type=jnp.float32)
    projected = projected.reshape(window_count, length, 3, head_count, head_size)
    queries = unit_rows(projected[:, :, 0]).astype(jnp.bfloat16)
    key_rows = unit_rows(projected[:, :, 1]).astype(jnp.bfloat16)
    values = projected[:, :, 2].astype(jnp.bfloat16)
    scores = jnp.einsum('wqhc,wkhc->whqk', queries.astype(jnp.float32), key_rows.astype(jnp.float32)) * scales[None, :, None, None]
    allowed = (labels[:, :, None] == labels[:, None, :])[:, None]
    weights = jnp.where(allowed, jnp.exp(scores), 0.0)
    probabilities = (weights / lax.optimization_barrier(jnp.sum(weights, axis=-1, keepdims=True))).astype(jnp.bfloat16)
    mixture = jnp.einsum('whqk,wkhc->wqhc', probabilities.astype(jnp.float32), values.astype(jnp.float32)).astype(jnp.bfloat16)
    attended = jnp.dot(mixture.reshape(window_count * length, feature_width), w_out, preferred_element_type=jnp.float32)
    residual_mid = windows + attended.reshape(window_count, length, feature_width)
    normed_two = layer_norm(residual_mid, gains[1]).astype(jnp.bfloat16)
    hidden = jax.nn.gelu(jnp.dot(normed_two.reshape(window_count * length, feature_width), w_upper, preferred_element_type=jnp.float32)).astype(jnp.bfloat16)
    lowered = jnp.dot(hidden, w_lower, preferred_element_type=jnp.float32)
    return residual_mid + lowered.reshape(window_count, length, feature_width)

def to_windows(lattice):
    level_count, row_count, col_count = lattice.shape[:3]
    trailing = lattice.shape[3:]
    blocked = lattice.reshape((level_count // WIN_LEV, WIN_LEV, row_count // WIN_LAT, WIN_LAT, col_count // WIN_LON, WIN_LON) + trailing)
    axis_order = (0, 2, 4, 1, 3, 5) + tuple(range(6, 6 + len(trailing)))
    return blocked.transpose(axis_order).reshape((-1, WIN_LEV * WIN_LAT * WIN_LON) + trailing)

def from_windows(windows, level_count, row_count, col_count):
    trailing = windows.shape[2:]
    blocked = windows.reshape((level_count // WIN_LEV, row_count // WIN_LAT, col_count // WIN_LON, WIN_LEV, WIN_LAT, WIN_LON) + trailing)
    axis_order = (0, 3, 1, 4, 2, 5) + tuple(range(6, 6 + len(trailing)))
    return blocked.transpose(axis_order).reshape((level_count, row_count, col_count) + trailing)

def region_labels(level_count, row_start, row_count, total_rows, col_count):
    level_ids = jnp.arange(level_count, dtype=jnp.int32)
    level_part = (level_ids >= level_count - WIN_LEV).astype(jnp.int32) + (level_ids >= level_count - WIN_LEV // 2).astype(jnp.int32)
    row_ids = jnp.mod(row_start + jnp.arange(row_count, dtype=jnp.int32), total_rows)
    row_part = (row_ids >= total_rows - WIN_LAT).astype(jnp.int32) + (row_ids >= total_rows - WIN_LAT // 2).astype(jnp.int32)
    return jnp.broadcast_to(level_part[:, None, None] * 3 + row_part[None, :, None], (level_count, row_count, col_count))

def grid_block(lattice, labels, w_attn_in, w_attn_out, w_up, w_down, norm_gains, logit_scales, block_index):
    windows = to_windows(lattice)
    label_windows = to_windows(labels)
    groups = windows.reshape((-1, 16) + windows.shape[1:])
    label_groups = label_windows.reshape((-1, 16) + label_windows.shape[1:])

    def group_step(members):
        return swin_block(members[0], members[1], w_attn_in[block_index], w_attn_out[block_index], w_up[block_index], w_down[block_index], norm_gains[block_index], logit_scales[block_index])
    result = lax.map(jax.checkpoint(group_step), (groups, label_groups))
    return from_windows(result.reshape(windows.shape), lattice.shape[0], lattice.shape[1], lattice.shape[2])

def reference(x_first, x_second, cotangent, w_attn_in, w_attn_out, w_up, w_down, norm_gains, logit_scales):
    shifts = (-(WIN_LEV // 2), -(WIN_LAT // 2), -(WIN_LON // 2))
    backs = (WIN_LEV // 2, WIN_LAT // 2, WIN_LON // 2)
    labels_two = region_labels(LEVELS, 0, NLAT, NLAT, NLON)
    labels_one = jnp.zeros((LEVELS, NLAT, NLON), jnp.int32)
    rolled_input = jnp.roll(x_second.astype(jnp.float32), shifts, axis=(0, 1, 2))
    rolled_cot = jnp.roll(cotangent.astype(jnp.float32), shifts, axis=(0, 1, 2))

    def second_block(lattice):
        return grid_block(lattice, labels_two, w_attn_in, w_attn_out, w_up, w_down, norm_gains, logit_scales, 1)

    def first_block(lattice):
        return grid_block(lattice, labels_one, w_attn_in, w_attn_out, w_up, w_down, norm_gains, logit_scales, 0)
    unused_two, pullback_two = jax.vjp(second_block, rolled_input)
    grad_rolled = pullback_two(rolled_cot)[0]
    grad_second = jnp.roll(grad_rolled, backs, axis=(0, 1, 2))
    unused_one, pullback_one = jax.vjp(first_block, x_first.astype(jnp.float32))
    grad_first = pullback_one(grad_second)[0]
    return (grad_first, grad_second)
```

```python
import functools
import math

import jax
import jax.numpy as jnp
from jax import lax
from jax.experimental import pallas as pl
from jax.experimental.pallas import tpu as pltpu
from jax.sharding import PartitionSpec as P

F32 = jnp.float32
BF = jnp.bfloat16
MESH = pl.DeviceIdType.MESH

LV, RW, CL = 4, 6, 12
HR, HC = RW // 2, CL // 2
QT = HR * HC
NT = LV * RW * CL
WT = NT // 2
QN = LV * QT
D, FF, HEADS, HD = 512, 2048, 8, 64
PAIRS = HEADS // 2
EPS = 1e-05
QUADS = ((1, 1), (1, 0), (0, 1), (0, 0))
ORDER = ((0, 1, 2, 3), (1, 2, 3, 0))
QPAD = 80

C0 = math.sqrt(2.0 / math.pi)
C1 = 0.044715


def nn(a, b):
    return lax.dot_general(a, b, (((1,), (0,)), ((), ())), preferred_element_type=F32)


def nt(a, b):
    return lax.dot_general(a, b, (((1,), (1,)), ((), ())), preferred_element_type=F32)


def tn(a, b):
    return lax.dot_general(a, b, (((0,), (0,)), ((), ())), preferred_element_type=F32)


def row_chunks(size=48):
    return [slice(i, i + size) for i in range(0, NT, size)]


def kernel(
    lat_n, lon_n,
    x1_in, x2_in, ct_in, win_in, wout_in, wup_in, wdn_in, gains, scales,
    g1_out, g2_out,
    tiles, win, wout, wup, wdn,
    tmp, quad, xf, dyf, xh1, rstd1, xh2, rstd2, nb, qk, vv, rs, aa, rr, oo, gp,
    rf, dyb, du, dr, drb, dob, dqk, dp, dn, allow, bd, res,
    sbuf, rbuf, gsbuf, grbuf,
    in_sem, w_sem, out_sem, ssem, rsem,
):
    a = lax.axis_index("lat")
    b = lax.axis_index("lon")
    up, down = lax.rem(a + 1, lat_n), lax.rem(a + lat_n - 1, lat_n)
    east, west = lax.rem(b + 1, lon_n), lax.rem(b + lon_n - 1, lon_n)
    before = ((a, west), (down, b), (down, west))
    after = ((a, east), (up, b), (up, east))

    loads = [
        pltpu.make_async_copy(src, tiles.at[i], in_sem.at[i])
        for i, src in enumerate((x2_in, ct_in, x1_in))
    ]
    for c in loads:
        c.start()
    weights = {}
    for n, (name, blk) in enumerate(
        (("in", 0), ("out", 0), ("up", 0), ("in", 1), ("out", 1), ("up", 1), ("dn", 1), ("dn", 0))
    ):
        src, dst = {"in": (win_in, win), "out": (wout_in, wout), "up": (wup_in, wup), "dn": (wdn_in, wdn)}[name]
        weights[name, blk] = pltpu.make_async_copy(src.at[blk], dst.at[blk], w_sem.at[n])
        weights[name, blk].start()

    barrier = pltpu.get_barrier_semaphore()
    for dev in before + after:
        pl.semaphore_signal(barrier, inc=1, device_id=dev, device_id_type=MESH)

    def load_tile(i):
        loads[i].wait()
        tmp[...] = tiles[i].reshape(LV * RW, CL, D).astype(F32)

    def piece(lev, row, q):
        rq, cq = QUADS[q]
        return tmp[lev * RW + HR * rq + row, HC * cq:HC * cq + HC, :]

    def pack_out(i):
        load_tile(i)
        for q in (1, 2, 3):
            for m, lev in enumerate(ORDER[1]):
                for row in range(HR):
                    o = m * QT + row * HC
                    quad[q, o:o + HC, :] = piece(lev, row, q)
            sbuf[i, q - 1, 0:QN, :] = quad[q].astype(BF)

    def keep_own(dst):
        for m, lev in enumerate(ORDER[1]):
            w, h = divmod(m, 2)
            for row in range(HR):
                o = w * WT + h * QT + row * HC
                dst[o:o + HC, :] = piece(lev, row, 0)

    def send(i, src, dst, devs, base):
        out = []
        for j, dev in enumerate(devs):
            s = base + j
            c = pltpu.make_async_remote_copy(
                src_ref=src.at[j], dst_ref=dst.at[j], send_sem=ssem.at[s], recv_sem=rsem.at[s],
                device_id=dev, device_id_type=MESH,
            )
            c.start()
            out.append(c)
        return out

    pack_out(0)
    keep_own(xf.at[1])
    pl.semaphore_wait(barrier, 6)
    sent_x = send(0, sbuf.at[0], rbuf.at[0], before, 0)
    pack_out(1)
    keep_own(dyf.at[1])
    sent_c = send(1, sbuf.at[1], rbuf.at[1], before, 3)

    load_tile(2)
    for q in range(4):
        for m, lev in enumerate(ORDER[0]):
            w, h = divmod(m, 2)
            for row in range(HR):
                o = w * WT + q * 2 * QT + h * QT + row * HC
                xf[0, o:o + HC, :] = piece(lev, row, q)

    ri = lax.broadcasted_iota(jnp.int32, (256, 256), 0)
    ci = lax.broadcasted_iota(jnp.int32, (256, 256), 1)
    bd[...] = (lax.shift_right_logical(ri, 6) == lax.shift_right_logical(ci, 6)).astype(F32).astype(BF)
    last_band = (a == lat_n - 1).astype(jnp.int32)
    for w in range(2):
        labels = []
        for axis in (0, 1):
            t = lax.broadcasted_iota(jnp.int32, (WT, WT), axis)
            lab = 2 * last_band * (t >= 2 * 2 * QT).astype(jnp.int32)
            if w == 1:
                for step in range(1, 8):
                    sign = 1 if step % 2 else -1
                    lab = lab + sign * (t >= QT * step).astype(jnp.int32)
            labels.append(lab)
        allow[w] = (labels[0] == labels[1]).astype(F32)
    lane = lax.broadcasted_iota(jnp.int32, (WT, 128), 1)
    first_half = lane < HD
    m_a = first_half.astype(F32).astype(BF)
    m_b = (lane >= HD).astype(F32).astype(BF)
    ones = jnp.ones((WT, 128), BF)

    def stacked(v):
        return jnp.concatenate([v * m_a, v * m_b], axis=0)

    def wide(r):
        return jnp.concatenate([r, r[:, :WT - 128]], axis=1)

    def layer_norm(src, gain, xh, rstd):
        for s in row_chunks():
            x = src[s, :]
            c = x - jnp.mean(x, axis=-1, keepdims=True)
            inv = lax.rsqrt(jnp.mean(c * c, axis=-1, keepdims=True) + EPS)
            h = c * inv
            xh[s, :] = h
            rstd[s, :] = jnp.broadcast_to(inv, (h.shape[0], 128))
            nb[s, :] = (h * gain).astype(BF)

    def layer_norm_back(base, grad, gain, xh, rstd, dst, dst_bf=None):
        for s in row_chunks():
            g = grad[s, :] * gain
            h = xh[s, :]
            m1 = jnp.mean(g, axis=-1, keepdims=True)
            m2 = jnp.mean(g * h, axis=-1, keepdims=True)
            inv = rstd[s, 0:1]
            v = base[s, :] + inv * (g - m1 - h * m2)
            dst[s, :] = v
            if dst_bf is not None:
                dst_bf[s, :] = v.astype(BF)

    def forward(k):
        x = xf.at[k]
        layer_norm(x, gains[2 * k:2 * k + 1, :], xh1.at[k], rstd1.at[k])
        weights["in", k].wait()
        n1 = nb[...]
        for j in range(6):
            c = slice(256 * j, 256 * j + 256)
            p = nn(n1, win[k, :, c])
            if j < 4:
                inv = lax.rsqrt(nn((p * p).astype(BF), bd[...]) + 1e-06)
                rs[k, :, c] = inv
                qk[k, :, c] = (p * inv).astype(BF)
            else:
                vv[k, :, 256 * (j - 4):256 * (j - 4) + 256] = p.astype(BF)
        for w in range(2):
            rows = slice(WT * w, WT * w + WT)
            for pr in range(PAIRS):
                it = w * PAIRS + pr
                c = slice(128 * pr, 128 * pr + 128)
                ck = slice(D + 128 * pr, D + 128 * pr + 128)
                qs = stacked(qk[k, rows, c])
                s = nt(qs, qk[k, rows, ck])
                ea = jnp.exp(s[:WT] * scales[k, 2 * pr])
                eb = jnp.exp(s[WT:] * scales[k, 2 * pr + 1])
                if k == 1:
                    ea = ea * allow[w]
                    eb = eb * allow[w]
                e = jnp.concatenate([ea, eb], axis=0).astype(BF)
                aa[k, it] = e
                ou = nn(e, jnp.concatenate([vv[k, rows, c], ones], axis=1))
                r = 1.0 / ou[:, 128:]
                rr[k, it] = r
                on = ou[:, :128] * r
                oo[k, rows, c] = jnp.where(first_half, on[:WT], on[WT:]).astype(BF)
        weights["out", k].wait()
        o = oo[k]
        for j in range(2):
            c = slice(256 * j, 256 * j + 256)
            rf[:, c] = x[:, c] + nn(o, wout[k, :, c])
        layer_norm(rf, gains[2 * k + 1:2 * k + 2, :], xh2.at[k], rstd2.at[k])
        weights["up", k].wait()
        n2 = nb[...]
        for j in range(8):
            c = slice(256 * j, 256 * j + 256)
            u = nn(n2, wup[k, :, c])
            u2 = u * u
            t = jnp.tanh(u * (C0 + (C0 * C1) * u2))
            gp[k, :, c] = (0.5 + 0.5 * t) + (1.0 - t * t) * (u * (0.5 * C0 + (1.5 * C0 * C1) * u2))

    def backward(k):
        dy = dyf.at[k]
        for s in row_chunks():
            dyb[s, :] = dy[s, :].astype(BF)
        weights["dn", k].wait()
        g = dyb[...]
        for j in range(8):
            c = slice(256 * j, 256 * j + 256)
            du[:, c] = (nt(g, wdn[k, c, :]) * gp[k, :, c]).astype(BF)
        g = du[...]
        for j in range(2):
            c = slice(256 * j, 256 * j + 256)
            dn[:, c] = nt(g, wup[k, c, :])
        layer_norm_back(dy, dn, gains[2 * k + 1:2 * k + 2, :], xh2.at[k], rstd2.at[k], dr, drb)
        g = drb[...]
        for j in range(2):
            c = slice(256 * j, 256 * j + 256)
            dob[:, c] = nt(g, wout[k, c, :]).astype(BF)
        for w in range(2):
            rows = slice(WT * w, WT * w + WT)
            for pr in range(PAIRS):
                it = w * PAIRS + pr
                c = slice(128 * pr, 128 * pr + 128)
                ck = slice(D + 128 * pr, D + 128 * pr + 128)
                q, kk, v = qk[k, rows, c], qk[k, rows, ck], vv[k, rows, c]
                do = dob[rows, c]
                prod = do.astype(F32) * oo[k, rows, c].astype(F32)
                da = jnp.sum(jnp.where(first_half, prod, 0.0), axis=-1, keepdims=True)
                db = jnp.sum(jnp.where(first_half, 0.0, prod), axis=-1, keepdims=True)
                dos = stacked(do)
                dpr = nt(dos, v)
                e = aa[k, it]
                r = rr[k, it]
                ra = wide(r[:WT] * scales[k, 2 * pr])
                rb = wide(r[WT:] * scales[k, 2 * pr + 1])
                e32 = e.astype(F32)
                dsa = e32[:WT] * ra * (dpr[:WT] - da)
                dsb = e32[WT:] * rb * (dpr[WT:] - db)
                ds = jnp.concatenate([dsa, dsb], axis=0).astype(BF)
                dq = nn(ds, kk)
                dqk[rows, c] = jnp.where(first_half, dq[:WT], dq[WT:]).astype(BF)
                dqk[rows, ck] = tn(ds, stacked(q)).astype(BF)
                dor = (dos.astype(F32) * r).astype(BF)
                dp[rows, 2 * D + 128 * pr:2 * D + 128 * pr + 128] = tn(e, dor).astype(BF)
        for j in range(4):
            c = slice(256 * j, 256 * j + 256)
            g = dqk[:, c].astype(F32)
            h = qk[k, :, c].astype(F32)
            dot = nn((g * h).astype(BF), bd[...])
            dp[:, c] = (rs[k, :, c] * (g - h * dot)).astype(BF)
        g = dp[...]
        for j in range(2):
            c = slice(256 * j, 256 * j + 256)
            dn[:, c] = nt(g, win[k, c, :])
        layer_norm_back(dr, dn, gains[2 * k:2 * k + 1, :], xh1.at[k], rstd1.at[k], rf)

    forward(0)

    def unpack_in(i, copies, dst):
        for j, c in enumerate(copies):
            c.wait_recv()
            quad[j + 1] = rbuf[i, j, 0:QN, :].astype(F32)
            for w in range(2):
                o = w * WT + (j + 1) * 2 * QT
                dst[o:o + 2 * QT, :] = quad[j + 1, w * 2 * QT:(w + 1) * 2 * QT, :]

    unpack_in(0, sent_x, xf.at[1])
    forward(1)
    unpack_in(1, sent_c, dyf.at[1])
    backward(1)

    for q in range(4):
        for w in range(2):
            o = w * WT + q * 2 * QT
            quad[q, w * 2 * QT:(w + 1) * 2 * QT, :] = rf[o:o + 2 * QT, :]
        if q:
            gsbuf[q - 1, 0:QN, :] = quad[q].astype(BF)
    sent_g = send(2, gsbuf, grbuf, after, 6)
    for q in range(4):
        if q:
            sent_g[q - 1].wait_recv()
            quad[q] = grbuf[q - 1, 0:QN, :].astype(F32)
        rq, cq = QUADS[q]
        for m, lev in enumerate(ORDER[1]):
            for row in range(HR):
                o = m * QT + row * HC
                res[1, lev, HR * rq + row, HC * cq:HC * cq + HC, :] = quad[q, o:o + HC, :]
            w, h = divmod(lev, 2)
            o = w * WT + q * 2 * QT + h * QT
            dyf[0, o:o + QT, :] = quad[q, m * QT:(m + 1) * QT, :]
    out2 = pltpu.make_async_copy(res.at[1], g2_out, out_sem.at[1])
    out2.start()
    backward(0)
    for q in range(4):
        rq, cq = QUADS[q]
        for lev in range(LV):
            w, h = divmod(lev, 2)
            for row in range(HR):
                o = w * WT + q * 2 * QT + h * QT + row * HC
                res[0, lev, HR * rq + row, HC * cq:HC * cq + HC, :] = rf[o:o + HC, :]
    out1 = pltpu.make_async_copy(res.at[0], g1_out, out_sem.at[0])
    out1.start()
    for c in sent_x + sent_c + sent_g:
        c.wait_send()
    out2.wait()
    out1.wait()


def per_device(x_first, x_second, cotangent, w_attn_in, w_attn_out, w_up, w_down, norm_gains, logit_scales):
    any_spec = pl.BlockSpec(memory_space=pl.ANY)
    tile = (LV, RW, CL, D)
    v = pltpu.VMEM
    scratch = [
        v((3,) + tile, BF), v((2, D, 3 * D), BF), v((2, D, D), BF), v((2, D, FF), BF), v((2, FF, D), BF),
        v((LV * RW, CL, D), F32), v((4, QN, D), F32), v((2, NT, D), F32), v((2, NT, D), F32),
        v((2, NT, D), F32), v((2, NT, 128), F32), v((2, NT, D), F32), v((2, NT, 128), F32),
        v((NT, D), BF), v((2, NT, 2 * D), BF), v((2, NT, D), BF), v((2, NT, 2 * D), F32),
        v((2, 2 * PAIRS, 2 * WT, WT), BF), v((2, 2 * PAIRS, 2 * WT, 128), F32), v((2, NT, D), BF), v((2, NT, FF), F32),
        v((NT, D), F32), v((NT, D), BF), v((NT, FF), BF), v((NT, D), F32), v((NT, D), BF), v((NT, D), BF),
        v((NT, 2 * D), BF), v((NT, 3 * D), BF), v((NT, D), F32), v((2, WT, WT), F32), v((256, 256), BF),
        v((2,) + tile, F32),
        v((2, 3, QPAD, D), BF), v((2, 3, QPAD, D), BF), v((3, QPAD, D), BF), v((3, QPAD, D), BF),
        pltpu.SemaphoreType.DMA((3,)), pltpu.SemaphoreType.DMA((8,)), pltpu.SemaphoreType.DMA((2,)),
        pltpu.SemaphoreType.DMA((9,)), pltpu.SemaphoreType.DMA((9,)),
    ]
    body = functools.partial(kernel, lax.axis_size("lat"), lax.axis_size("lon"))
    return pl.pallas_call(
        body,
        out_shape=(jax.ShapeDtypeStruct(tile, F32), jax.ShapeDtypeStruct(tile, F32)),
        in_specs=[any_spec] * 7 + [pl.BlockSpec(memory_space=pltpu.VMEM), pl.BlockSpec(memory_space=pltpu.SMEM)],
        out_specs=(any_spec, any_spec),
        scratch_shapes=scratch,
        compiler_params=pltpu.CompilerParams(
            collective_id=0, has_side_effects=True, vmem_limit_bytes=60 * 1024 * 1024
        ),
        name="step",
    )(
        x_first, x_second, cotangent, w_attn_in, w_attn_out, w_up, w_down,
        norm_gains.reshape(4, D), logit_scales,
    )


def solution(mesh):
    grid = P(None, "lat", "lon", None)
    return jax.shard_map(
        per_device,
        mesh=mesh,
        in_specs=(grid, grid, grid, P(), P(), P(), P(), P(), P()),
        out_specs=(grid, grid),
        check_vma=False,
    )
```

```python
import functools
import math

import jax
import jax.numpy as jnp
from jax import lax
from jax.experimental import pallas as pl
from jax.experimental.pallas import tpu as pltpu
from jax.sharding import PartitionSpec as P

F32 = jnp.float32
BF = jnp.bfloat16
MESH = pl.DeviceIdType.MESH

LV, RW, CL = 4, 6, 12
HR, HC = RW // 2, CL // 2
RC = RW * CL
NT = LV * RW * CL
WT = NT // 2
D, FF, HEADS, HD = 512, 2048, 8, 64
PAIRS = HEADS // 2
EPS = 1e-05
QUADS = ((1, 1), (1, 0), (0, 1), (0, 0))
ORDER = ((0, 1, 2, 3), (1, 2, 3, 0))

C0 = math.sqrt(2.0 / math.pi)
C1 = 0.044715


def nn(a, b):
    return lax.dot_general(a, b, (((1,), (0,)), ((), ())), preferred_element_type=F32)


def nt(a, b):
    return lax.dot_general(a, b, (((1,), (1,)), ((), ())), preferred_element_type=F32)


def tn(a, b):
    return lax.dot_general(a, b, (((0,), (0,)), ((), ())), preferred_element_type=F32)


def row_chunks(size=48):
    return [slice(i, i + size) for i in range(0, NT, size)]


def kernel(
    lat_n, lon_n,
    x1_in, x2_in, ct_in, win_in, wout_in, wup_in, wdn_in, gains, scales,
    g1_out, g2_out,
    tiles, win, wout, wup, wdn,
    moved, flat, xf, dyf, xh1, rstd1, xh2, rstd2, nb, qk, vv, rs, aa, rr, oo, gp,
    rf, dyb, du, dr, drb, dob, dqk, dp, dn, allow, bd, res,
    gsend, grecv,
    in_sem, w_sem, out_sem, ssem, rsem,
):
    a = lax.axis_index("lat")
    b = lax.axis_index("lon")
    up, down = lax.rem(a + 1, lat_n), lax.rem(a + lat_n - 1, lat_n)
    east, west = lax.rem(b + 1, lon_n), lax.rem(b + lon_n - 1, lon_n)
    before = ((a, west), (down, b), (down, west))
    after = ((a, east), (up, b), (up, east))

    barrier = pltpu.get_barrier_semaphore()
    for dev in before + after:
        pl.semaphore_signal(barrier, inc=1, device_id=dev, device_id_type=MESH)

    loads = [
        pltpu.make_async_copy(x2_in, tiles.at[0], in_sem.at[0]),
        pltpu.make_async_copy(ct_in, tiles.at[1], in_sem.at[1]),
        pltpu.make_async_copy(x1_in, tiles.at[2], in_sem.at[2]),
        pltpu.make_async_copy(x2_in.at[HR:RW, HC:CL], moved.at[0, 0:HR, 0:HC], in_sem.at[3]),
        pltpu.make_async_copy(ct_in.at[HR:RW, HC:CL], moved.at[1, 0:HR, 0:HC], in_sem.at[4]),
    ]
    for c in loads:
        c.start()
    weights = {}
    for n, (name, blk) in enumerate(
        (("in", 0), ("out", 0), ("up", 0), ("in", 1), ("out", 1), ("up", 1), ("dn", 1), ("dn", 0))
    ):
        src, dst = {"in": (win_in, win), "out": (wout_in, wout), "up": (wup_in, wup), "dn": (wdn_in, wdn)}[name]
        weights[name, blk] = pltpu.make_async_copy(src.at[blk], dst.at[blk], w_sem.at[n])
        weights[name, blk].start()

    def spots(half):
        rq, cq = half
        return [(r, c) for r in range(HR * rq, HR * rq + HR) for c in range(HC * cq, HC * cq + HC)]

    def at(r, c):
        o = LV * (r * CL + c)
        return slice(o, o + LV)

    def levels_apart(dst, order):
        for m, lev in enumerate(order):
            for j in range(D // 128):
                dst[m * RC:m * RC + RC, 128 * j:128 * j + 128] = flat[j, pl.ds(lev, RC, stride=LV), :]

    def levels_together(src, order):
        for m, lev in enumerate(order):
            for j in range(D // 128):
                flat[j, pl.ds(lev, RC, stride=LV), :] = src[m * RC:m * RC + RC, 128 * j:128 * j + 128]

    def set_flat(r, c, v):
        for j in range(D // 128):
            flat[j, at(r, c), :] = v[:, 128 * j:128 * j + 128]

    def get_flat(r, c):
        return jnp.concatenate([flat[j, at(r, c), :] for j in range(D // 128)], axis=1)

    def from_tile(tile, dst, order):
        for r in range(RW):
            for c in range(CL):
                set_flat(r, c, tile[r, c].astype(F32))
        levels_apart(dst, order)

    def block_of(ref, half):
        rq, cq = half
        return ref.at[HR * rq:HR * rq + HR, HC * cq:HC * cq + HC]

    def swapped(half):
        return (1 - half[0], 1 - half[1])

    def send(src, dst, half, dev, n):
        c = pltpu.make_async_remote_copy(
            src_ref=block_of(src, half), dst_ref=block_of(dst, swapped(half)),
            send_sem=ssem.at[n], recv_sem=rsem.at[n], device_id=dev, device_id_type=MESH,
        )
        c.start()
        return c

    loads[2].wait()
    from_tile(tiles.at[2], xf.at[0], ORDER[0])
    loads[0].wait()
    pl.semaphore_wait(barrier, 6)
    sent_x = [send(tiles.at[0], moved.at[0], QUADS[q], before[q - 1], q - 1) for q in (3, 2, 1)]
    loads[1].wait()
    sent_c = [send(tiles.at[1], moved.at[1], QUADS[q], before[q - 1], q + 2) for q in (3, 2, 1)]

    ri = lax.broadcasted_iota(jnp.int32, (256, 256), 0)
    ci = lax.broadcasted_iota(jnp.int32, (256, 256), 1)
    bd[...] = (lax.shift_right_logical(ri, 6) == lax.shift_right_logical(ci, 6)).astype(F32).astype(BF)
    last_band = (a == lat_n - 1).astype(jnp.int32)
    for w in range(2):
        labels = []
        for axis in (0, 1):
            t = lax.broadcasted_iota(jnp.int32, (WT, WT), axis)
            second = (t >= RC).astype(jnp.int32)
            late_rows = (t - RC * second >= RC // 2).astype(jnp.int32)
            lab = 2 * last_band * late_rows
            if w == 1:
                lab = lab + second
            labels.append(lab)
        allow[w] = (labels[0] == labels[1]).astype(F32)
    lane = lax.broadcasted_iota(jnp.int32, (WT, 128), 1)
    first_half = lane < HD
    m_a = first_half.astype(F32).astype(BF)
    m_b = (lane >= HD).astype(F32).astype(BF)
    ones = jnp.ones((WT, 128), BF)

    def stacked(v):
        return jnp.concatenate([v * m_a, v * m_b], axis=0)

    def wide(r):
        return jnp.concatenate([r, r[:, :WT - 128]], axis=1)

    def layer_norm(src, gain, xh, rstd):
        for s in row_chunks():
            x = src[s, :]
            c = x - jnp.mean(x, axis=-1, keepdims=True)
            inv = lax.rsqrt(jnp.mean(c * c, axis=-1, keepdims=True) + EPS)
            h = c * inv
            xh[s, :] = h
            rstd[s, :] = jnp.broadcast_to(inv, (h.shape[0], 128))
            nb[s, :] = (h * gain).astype(BF)

    def layer_norm_back(base, grad, gain, xh, rstd, dst, dst_bf=None):
        for s in row_chunks():
            g = grad[s, :] * gain
            h = xh[s, :]
            m1 = jnp.mean(g, axis=-1, keepdims=True)
            m2 = jnp.mean(g * h, axis=-1, keepdims=True)
            inv = rstd[s, 0:1]
            v = base[s, :] + inv * (g - m1 - h * m2)
            dst[s, :] = v
            if dst_bf is not None:
                dst_bf[s, :] = v.astype(BF)

    def forward(k):
        x = xf.at[k]
        layer_norm(x, gains[k, 0:1, :], xh1.at[k], rstd1.at[k])
        weights["in", k].wait()
        n1 = nb[...]
        for j in range(6):
            c = slice(256 * j, 256 * j + 256)
            p = nn(n1, win[k, :, c])
            if j < 4:
                inv = lax.rsqrt(nn((p * p).astype(BF), bd[...]) + 1e-06)
                rs[k, :, c] = inv
                qk[k, :, c] = (p * inv).astype(BF)
            else:
                vv[k, :, 256 * (j - 4):256 * (j - 4) + 256] = p.astype(BF)
        for w in range(2):
            rows = slice(WT * w, WT * w + WT)
            for pr in range(PAIRS):
                it = w * PAIRS + pr
                c = slice(128 * pr, 128 * pr + 128)
                ck = slice(D + 128 * pr, D + 128 * pr + 128)
                qs = stacked(qk[k, rows, c])
                s = nt(qs, qk[k, rows, ck])
                ea = jnp.exp(s[:WT] * scales[k, 2 * pr])
                eb = jnp.exp(s[WT:] * scales[k, 2 * pr + 1])
                if k == 1:
                    ea = ea * allow[w]
                    eb = eb * allow[w]
                e = jnp.concatenate([ea, eb], axis=0).astype(BF)
                aa[k, it] = e
                ou = nn(e, jnp.concatenate([vv[k, rows, c], ones], axis=1))
                r = 1.0 / ou[:, 128:]
                rr[k, it] = r
                on = ou[:, :128] * r
                oo[k, rows, c] = jnp.where(first_half, on[:WT], on[WT:]).astype(BF)
        weights["out", k].wait()
        o = oo[k]
        for j in range(2):
            c = slice(256 * j, 256 * j + 256)
            rf[:, c] = x[:, c] + nn(o, wout[k, :, c])
        layer_norm(rf, gains[k, 1:2, :], xh2.at[k], rstd2.at[k])
        weights["up", k].wait()
        n2 = nb[...]
        for j in range(8):
            c = slice(256 * j, 256 * j + 256)
            u = nn(n2, wup[k, :, c])
            u2 = u * u
            t = jnp.tanh(u * (C0 + (C0 * C1) * u2))
            gp[k, :, c] = (0.5 + 0.5 * t) + (1.0 - t * t) * (u * (0.5 * C0 + (1.5 * C0 * C1) * u2))

    def backward(k):
        dy = dyf.at[k]
        for s in row_chunks():
            dyb[s, :] = dy[s, :].astype(BF)
        weights["dn", k].wait()
        g = dyb[...]
        for j in range(8):
            c = slice(256 * j, 256 * j + 256)
            du[:, c] = (nt(g, wdn[k, c, :]) * gp[k, :, c]).astype(BF)
        g = du[...]
        for j in range(2):
            c = slice(256 * j, 256 * j + 256)
            dn[:, c] = nt(g, wup[k, c, :])
        layer_norm_back(dy, dn, gains[k, 1:2, :], xh2.at[k], rstd2.at[k], dr, drb)
        g = drb[...]
        for j in range(2):
            c = slice(256 * j, 256 * j + 256)
            dob[:, c] = nt(g, wout[k, c, :]).astype(BF)
        for w in range(2):
            rows = slice(WT * w, WT * w + WT)
            for pr in range(PAIRS):
                it = w * PAIRS + pr
                c = slice(128 * pr, 128 * pr + 128)
                ck = slice(D + 128 * pr, D + 128 * pr + 128)
                q, kk, v = qk[k, rows, c], qk[k, rows, ck], vv[k, rows, c]
                do = dob[rows, c]
                prod = do.astype(F32) * oo[k, rows, c].astype(F32)
                da = jnp.sum(jnp.where(first_half, prod, 0.0), axis=-1, keepdims=True)
                db = jnp.sum(jnp.where(first_half, 0.0, prod), axis=-1, keepdims=True)
                dos = stacked(do)
                dpr = nt(dos, v)
                e = aa[k, it]
                r = rr[k, it]
                ra = wide(r[:WT] * scales[k, 2 * pr])
                rb = wide(r[WT:] * scales[k, 2 * pr + 1])
                e32 = e.astype(F32)
                dsa = e32[:WT] * ra * (dpr[:WT] - da)
                dsb = e32[WT:] * rb * (dpr[WT:] - db)
                ds = jnp.concatenate([dsa, dsb], axis=0).astype(BF)
                dq = nn(ds, kk)
                dqk[rows, c] = jnp.where(first_half, dq[:WT], dq[WT:]).astype(BF)
                dqk[rows, ck] = tn(ds, stacked(q)).astype(BF)
                dor = (dos.astype(F32) * r).astype(BF)
                dp[rows, 2 * D + 128 * pr:2 * D + 128 * pr + 128] = tn(e, dor).astype(BF)
        for j in range(4):
            c = slice(256 * j, 256 * j + 256)
            g = dqk[:, c].astype(F32)
            h = qk[k, :, c].astype(F32)
            dot = nn((g * h).astype(BF), bd[...])
            dp[:, c] = (rs[k, :, c] * (g - h * dot)).astype(BF)
        g = dp[...]
        for j in range(2):
            c = slice(256 * j, 256 * j + 256)
            dn[:, c] = nt(g, win[k, c, :])
        layer_norm_back(dr, dn, gains[k, 0:1, :], xh1.at[k], rstd1.at[k], rf)

    forward(0)

    loads[3].wait()
    for c in sent_x:
        c.wait_recv()
    from_tile(moved.at[0], xf.at[1], ORDER[1])
    forward(1)
    loads[4].wait()
    for c in sent_c:
        c.wait_recv()
    from_tile(moved.at[1], dyf.at[1], ORDER[1])
    backward(1)

    levels_together(rf, ORDER[1])
    sent_g = []
    for q in (3, 2, 1):
        for r, c in spots(swapped(QUADS[q])):
            gsend[r, c] = get_flat(r, c).astype(BF)
    for q in (3, 2, 1):
        sent_g.append(send(gsend, grecv, swapped(QUADS[q]), after[q - 1], q + 5))
    own = {(r + HR, c + HC): get_flat(r, c) for r, c in spots((0, 0))}
    for (r, c), v in own.items():
        set_flat(r, c, v)
        res[1, r, c] = v
    for q, copy in zip((3, 2, 1), sent_g):
        copy.wait_recv()
    for q in (3, 2, 1):
        for r, c in spots(QUADS[q]):
            v = grecv[r, c].astype(F32)
            set_flat(r, c, v)
            res[1, r, c] = v
    levels_apart(dyf.at[0], ORDER[0])
    out2 = pltpu.make_async_copy(res.at[1], g2_out, out_sem.at[1])
    out2.start()
    backward(0)
    levels_together(rf, ORDER[0])
    for r in range(RW):
        for c in range(CL):
            res[0, r, c] = get_flat(r, c)
    out1 = pltpu.make_async_copy(res.at[0], g1_out, out_sem.at[0])
    out1.start()
    for c in sent_x + sent_c + sent_g:
        c.wait_send()
    out2.wait()
    out1.wait()


def per_device(x_first, x_second, cotangent, w_attn_in, w_attn_out, w_up, w_down, norm_gains, logit_scales):
    any_spec = pl.BlockSpec(memory_space=pl.ANY)
    tile = (RW, CL, LV, D)
    v = pltpu.VMEM
    scratch = [
        v((3,) + tile, BF), v((2, D, 3 * D), BF), v((2, D, D), BF), v((2, D, FF), BF), v((2, FF, D), BF),
        v((2,) + tile, BF), v((D // 128, NT, 128), F32), v((2, NT, D), F32), v((2, NT, D), F32),
        v((2, NT, D), F32), v((2, NT, 128), F32), v((2, NT, D), F32), v((2, NT, 128), F32),
        v((NT, D), BF), v((2, NT, 2 * D), BF), v((2, NT, D), BF), v((2, NT, 2 * D), F32),
        v((2, 2 * PAIRS, 2 * WT, WT), BF), v((2, 2 * PAIRS, 2 * WT, 128), F32), v((2, NT, D), BF), v((2, NT, FF), F32),
        v((NT, D), F32), v((NT, D), BF), v((NT, FF), BF), v((NT, D), F32), v((NT, D), BF), v((NT, D), BF),
        v((NT, 2 * D), BF), v((NT, 3 * D), BF), v((NT, D), F32), v((2, WT, WT), F32), v((256, 256), BF),
        v((2,) + tile, F32),
        v(tile, BF), v(tile, BF),
        pltpu.SemaphoreType.DMA((5,)), pltpu.SemaphoreType.DMA((8,)), pltpu.SemaphoreType.DMA((2,)),
        pltpu.SemaphoreType.DMA((9,)), pltpu.SemaphoreType.DMA((9,)),
    ]
    body = functools.partial(kernel, lax.axis_size("lat"), lax.axis_size("lon"))
    cells = (1, 2, 0, 3)
    out = pl.pallas_call(
        body,
        out_shape=(jax.ShapeDtypeStruct(tile, F32), jax.ShapeDtypeStruct(tile, F32)),
        in_specs=[any_spec] * 7 + [pl.BlockSpec(memory_space=pltpu.VMEM), pl.BlockSpec(memory_space=pltpu.SMEM)],
        out_specs=(any_spec, any_spec),
        scratch_shapes=scratch,
        compiler_params=pltpu.CompilerParams(
            collective_id=0, has_side_effects=True, vmem_limit_bytes=60 * 1024 * 1024
        ),
        name="step",
    )(
        *[jnp.transpose(v, cells) for v in (x_first, x_second, cotangent)],
        w_attn_in, w_attn_out, w_up, w_down, norm_gains, logit_scales,
    )
    return tuple(jnp.transpose(v, (2, 0, 1, 3)) for v in out)


def solution(mesh):
    grid = P(None, "lat", "lon", None)
    return jax.shard_map(
        per_device,
        mesh=mesh,
        in_specs=(grid, grid, grid, P(), P(), P(), P(), P(), P()),
        out_specs=(grid, grid),
        check_vma=False,
    )
```

```python
import functools
import math

import jax
import jax.numpy as jnp
from jax import lax
from jax.experimental import pallas as pl
from jax.experimental.pallas import tpu as pltpu
from jax.sharding import PartitionSpec as P

F32 = jnp.float32
BF = jnp.bfloat16
MESH = pl.DeviceIdType.MESH

LV, RW, CL = 4, 6, 12
HR, HC = RW // 2, CL // 2
RC = RW * CL
NT = LV * RW * CL
WT = NT // 2
D, FF, HEADS, HD = 512, 2048, 8, 64
PAIRS = HEADS // 2
EPS = 1e-05
VMEM_LIMIT = 48 * 1024 * 1024
QUADS = ((1, 1), (1, 0), (0, 1), (0, 0))
ORDER = ((0, 1, 2, 3), (1, 2, 3, 0))

C0 = math.sqrt(2.0 / math.pi)
C1 = 0.044715


def nn(a, b):
    return lax.dot_general(a, b, (((1,), (0,)), ((), ())), preferred_element_type=F32)


def nt(a, b):
    return lax.dot_general(a, b, (((1,), (1,)), ((), ())), preferred_element_type=F32)


def tn(a, b):
    return lax.dot_general(a, b, (((0,), (0,)), ((), ())), preferred_element_type=F32)


def row_chunks(size=48):
    return [slice(i, i + size) for i in range(0, NT, size)]


def kernel(
    lat_n, lon_n,
    x1_in, x2_in, ct_in, win_in, wout_in, wup_in, wdn_in, gains_in, scales_in,
    g1_out, g2_out,
    tiles, win, wout, wup, wdn,
    moved, flat, xf, dyf, xh1, rstd1, xh2, rstd2, nb, qk, vv, rs, aa, rr, oo, gp,
    rf, dyb, du, dr, drb, dob, dqk, dp, dn, allow, bd,
    gsend, grecv, gains, scales,
    in_sem, w_sem, ssem, rsem,
):
    a = lax.axis_index("lat")
    b = lax.axis_index("lon")
    up, down = lax.rem(a + 1, lat_n), lax.rem(a + lat_n - 1, lat_n)
    east, west = lax.rem(b + 1, lon_n), lax.rem(b + lon_n - 1, lon_n)
    before = ((a, west), (down, b), (down, west))
    after = ((a, east), (up, b), (up, east))

    barrier = pltpu.get_barrier_semaphore()
    for dev in before + after:
        pl.semaphore_signal(barrier, inc=1, device_id=dev, device_id_type=MESH)

    loads = [
        pltpu.make_async_copy(x2_in, tiles.at[0], in_sem.at[0]),
        pltpu.make_async_copy(ct_in, tiles.at[1], in_sem.at[1]),
        pltpu.make_async_copy(x1_in, tiles.at[2], in_sem.at[2]),
        pltpu.make_async_copy(x2_in.at[HR:RW, HC:CL], moved.at[0, 0:HR, 0:HC], in_sem.at[3]),
        pltpu.make_async_copy(ct_in.at[HR:RW, HC:CL], moved.at[1, 0:HR, 0:HC], in_sem.at[4]),
        pltpu.make_async_copy(gains_in, gains, in_sem.at[5]),
        pltpu.make_async_copy(scales_in, scales, in_sem.at[6]),
    ]
    for i in (2, 0, 5, 6, 1, 3, 4):
        loads[i].start()
    weights = {}
    for n, (name, blk) in enumerate(
        (("in", 0), ("out", 0), ("up", 0), ("in", 1), ("out", 1), ("up", 1), ("dn", 1), ("dn", 0))
    ):
        src, dst = {"in": (win_in, win), "out": (wout_in, wout), "up": (wup_in, wup), "dn": (wdn_in, wdn)}[name]
        weights[name, blk] = pltpu.make_async_copy(src.at[blk], dst.at[blk], w_sem.at[n])

    def fetch(*names):
        for n in names:
            weights[n].start()

    fetch(("in", 0))

    def spots(half):
        rq, cq = half
        return [(r, c) for r in range(HR * rq, HR * rq + HR) for c in range(HC * cq, HC * cq + HC)]

    def at(r, c):
        o = LV * (r * CL + c)
        return slice(o, o + LV)

    def levels_apart(dst, order):
        for m, lev in enumerate(order):
            for j in range(D // 128):
                dst[m * RC:m * RC + RC, 128 * j:128 * j + 128] = flat[j, pl.ds(lev, RC, stride=LV), :]

    def levels_together(src, order):
        for m, lev in enumerate(order):
            for j in range(D // 128):
                flat[j, pl.ds(lev, RC, stride=LV), :] = src[m * RC:m * RC + RC, 128 * j:128 * j + 128]

    def set_flat(r, c, v):
        for j in range(D // 128):
            flat[j, at(r, c), :] = v[:, 128 * j:128 * j + 128]

    def get_flat(r, c):
        return jnp.concatenate([flat[j, at(r, c), :] for j in range(D // 128)], axis=1)

    def from_tile(tile, dst, order):
        for r in range(RW):
            for c in range(CL):
                set_flat(r, c, tile[r, c].astype(F32))
        levels_apart(dst, order)

    def block_of(ref, half):
        rq, cq = half
        return ref.at[HR * rq:HR * rq + HR, HC * cq:HC * cq + HC]

    def swapped(half):
        return (1 - half[0], 1 - half[1])

    def send(src, dst, half, dev, n):
        c = pltpu.make_async_remote_copy(
            src_ref=block_of(src, half), dst_ref=block_of(dst, swapped(half)),
            send_sem=ssem.at[n], recv_sem=rsem.at[n], device_id=dev, device_id_type=MESH,
        )
        c.start()
        return c

    loads[2].wait()
    from_tile(tiles.at[2], xf.at[0], ORDER[0])
    loads[0].wait()
    fetch(("out", 0), ("up", 0))
    loads[5].wait()
    loads[6].wait()
    pl.semaphore_wait(barrier, 6)
    sent_x = [send(tiles.at[0], moved.at[0], QUADS[q], before[q - 1], q - 1) for q in (3, 2, 1)]
    loads[1].wait()
    sent_c = [send(tiles.at[1], moved.at[1], QUADS[q], before[q - 1], q + 2) for q in (3, 2, 1)]

    ri = lax.broadcasted_iota(jnp.int32, (256, 256), 0)
    ci = lax.broadcasted_iota(jnp.int32, (256, 256), 1)
    bd[...] = (lax.shift_right_logical(ri, 6) == lax.shift_right_logical(ci, 6)).astype(F32).astype(BF)
    last_band = (a == lat_n - 1).astype(jnp.int32)
    for w in range(2):
        labels = []
        for axis in (0, 1):
            t = lax.broadcasted_iota(jnp.int32, (WT, WT), axis)
            second = (t >= RC).astype(jnp.int32)
            late_rows = (t - RC * second >= RC // 2).astype(jnp.int32)
            lab = 2 * last_band * late_rows
            if w == 1:
                lab = lab + second
            labels.append(lab)
        allow[w] = (labels[0] == labels[1]).astype(F32)
    lane = lax.broadcasted_iota(jnp.int32, (WT, 128), 1)
    first_half = lane < HD
    m_a = first_half.astype(F32).astype(BF)
    m_b = (lane >= HD).astype(F32).astype(BF)
    ones = jnp.ones((WT, 128), BF)

    def stacked(v):
        return jnp.concatenate([v * m_a, v * m_b], axis=0)

    def wide(r):
        return jnp.concatenate([r, r[:, :WT - 128]], axis=1)

    def layer_norm(src, gain, xh, rstd):
        for s in row_chunks():
            x = src[s, :]
            c = x - jnp.mean(x, axis=-1, keepdims=True)
            inv = lax.rsqrt(jnp.mean(c * c, axis=-1, keepdims=True) + EPS)
            h = c * inv
            xh[s, :] = h
            rstd[s, :] = jnp.broadcast_to(inv, (h.shape[0], 128))
            nb[s, :] = (h * gain).astype(BF)

    def layer_norm_back(base, grad, gain, xh, rstd, dst, dst_bf=None):
        for s in row_chunks():
            g = grad[s, :] * gain
            h = xh[s, :]
            m1 = jnp.mean(g, axis=-1, keepdims=True)
            m2 = jnp.mean(g * h, axis=-1, keepdims=True)
            inv = rstd[s, 0:1]
            v = base[s, :] + inv * (g - m1 - h * m2)
            dst[s, :] = v
            if dst_bf is not None:
                dst_bf[s, :] = v.astype(BF)

    def forward(k):
        x = xf.at[k]
        layer_norm(x, gains[k, 0:1, :], xh1.at[k], rstd1.at[k])
        weights["in", k].wait()
        if k == 0:
            fetch(("in", 1), ("out", 1), ("up", 1))
        n1 = nb[...]
        for j in range(6):
            c = slice(256 * j, 256 * j + 256)
            p = nn(n1, win[k, :, c])
            if j < 4:
                inv = lax.rsqrt(nn((p * p).astype(BF), bd[...]) + 1e-06)
                rs[k, :, c] = inv
                qk[k, :, c] = (p * inv).astype(BF)
            else:
                vv[k, :, 256 * (j - 4):256 * (j - 4) + 256] = p.astype(BF)
        for w in range(2):
            rows = slice(WT * w, WT * w + WT)
            for pr in range(PAIRS):
                it = w * PAIRS + pr
                c = slice(128 * pr, 128 * pr + 128)
                ck = slice(D + 128 * pr, D + 128 * pr + 128)
                qs = stacked(qk[k, rows, c])
                s = nt(qs, qk[k, rows, ck])
                ea = jnp.exp(s[:WT] * scales[k, 2 * pr])
                eb = jnp.exp(s[WT:] * scales[k, 2 * pr + 1])
                if k == 1:
                    ea = ea * allow[w]
                    eb = eb * allow[w]
                e = jnp.concatenate([ea, eb], axis=0).astype(BF)
                aa[k, it] = e
                ou = nn(e, jnp.concatenate([vv[k, rows, c], ones], axis=1))
                r = 1.0 / ou[:, 128:]
                rr[k, it] = r
                on = ou[:, :128] * r
                oo[k, rows, c] = jnp.where(first_half, on[:WT], on[WT:]).astype(BF)
        weights["out", k].wait()
        o = oo[k]
        for j in range(2):
            c = slice(256 * j, 256 * j + 256)
            rf[:, c] = x[:, c] + nn(o, wout[k, :, c])
        layer_norm(rf, gains[k, 1:2, :], xh2.at[k], rstd2.at[k])
        weights["up", k].wait()
        if k == 0:
            fetch(("dn", 1), ("dn", 0))
        n2 = nb[...]
        for j in range(8):
            c = slice(256 * j, 256 * j + 256)
            u = nn(n2, wup[k, :, c])
            u2 = u * u
            t = jnp.tanh(u * (C0 + (C0 * C1) * u2))
            gp[k, :, c] = (0.5 + 0.5 * t) + (1.0 - t * t) * (u * (0.5 * C0 + (1.5 * C0 * C1) * u2))

    def backward(k):
        dy = dyf.at[k]
        for s in row_chunks():
            dyb[s, :] = dy[s, :].astype(BF)
        weights["dn", k].wait()
        g = dyb[...]
        for j in range(8):
            c = slice(256 * j, 256 * j + 256)
            du[:, c] = (nt(g, wdn[k, c, :]) * gp[k, :, c]).astype(BF)
        g = du[...]
        for j in range(2):
            c = slice(256 * j, 256 * j + 256)
            dn[:, c] = nt(g, wup[k, c, :])
        layer_norm_back(dy, dn, gains[k, 1:2, :], xh2.at[k], rstd2.at[k], dr, drb)
        g = drb[...]
        for j in range(2):
            c = slice(256 * j, 256 * j + 256)
            dob[:, c] = nt(g, wout[k, c, :]).astype(BF)
        for w in range(2):
            rows = slice(WT * w, WT * w + WT)
            for pr in range(PAIRS):
                it = w * PAIRS + pr
                c = slice(128 * pr, 128 * pr + 128)
                ck = slice(D + 128 * pr, D + 128 * pr + 128)
                q, kk, v = qk[k, rows, c], qk[k, rows, ck], vv[k, rows, c]
                do = dob[rows, c]
                prod = do.astype(F32) * oo[k, rows, c].astype(F32)
                da = jnp.sum(jnp.where(first_half, prod, 0.0), axis=-1, keepdims=True)
                db = jnp.sum(jnp.where(first_half, 0.0, prod), axis=-1, keepdims=True)
                dos = stacked(do)
                dpr = nt(dos, v)
                e = aa[k, it]
                r = rr[k, it]
                ra = wide(r[:WT] * scales[k, 2 * pr])
                rb = wide(r[WT:] * scales[k, 2 * pr + 1])
                e32 = e.astype(F32)
                dsa = e32[:WT] * ra * (dpr[:WT] - da)
                dsb = e32[WT:] * rb * (dpr[WT:] - db)
                ds = jnp.concatenate([dsa, dsb], axis=0).astype(BF)
                dq = nn(ds, kk)
                dqk[rows, c] = jnp.where(first_half, dq[:WT], dq[WT:]).astype(BF)
                dqk[rows, ck] = tn(ds, stacked(q)).astype(BF)
                dor = (dos.astype(F32) * r).astype(BF)
                dp[rows, 2 * D + 128 * pr:2 * D + 128 * pr + 128] = tn(e, dor).astype(BF)
        for j in range(4):
            c = slice(256 * j, 256 * j + 256)
            g = dqk[:, c].astype(F32)
            h = qk[k, :, c].astype(F32)
            dot = nn((g * h).astype(BF), bd[...])
            dp[:, c] = (rs[k, :, c] * (g - h * dot)).astype(BF)
        g = dp[...]
        for j in range(2):
            c = slice(256 * j, 256 * j + 256)
            dn[:, c] = nt(g, win[k, c, :])
        layer_norm_back(dr, dn, gains[k, 0:1, :], xh1.at[k], rstd1.at[k], rf)

    forward(0)

    loads[3].wait()
    for c in sent_x:
        c.wait_recv()
    from_tile(moved.at[0], xf.at[1], ORDER[1])
    forward(1)
    loads[4].wait()
    for c in sent_c:
        c.wait_recv()
    from_tile(moved.at[1], dyf.at[1], ORDER[1])
    backward(1)

    levels_together(rf, ORDER[1])
    sent_g = []
    for q in (3, 2, 1):
        for r, c in spots(swapped(QUADS[q])):
            gsend[r, c] = get_flat(r, c).astype(BF)
    for q in (3, 2, 1):
        sent_g.append(send(gsend, grecv, swapped(QUADS[q]), after[q - 1], q + 5))
    own = {(r + HR, c + HC): get_flat(r, c) for r, c in spots((0, 0))}
    for (r, c), v in own.items():
        set_flat(r, c, v)
        g2_out[r, c] = v
    for q, copy in zip((3, 2, 1), sent_g):
        copy.wait_recv()
    for q in (3, 2, 1):
        for r, c in spots(QUADS[q]):
            v = grecv[r, c].astype(F32)
            set_flat(r, c, v)
            g2_out[r, c] = v
    levels_apart(dyf.at[0], ORDER[0])
    backward(0)
    levels_together(rf, ORDER[0])
    for r in range(RW):
        for c in range(CL):
            g1_out[r, c] = get_flat(r, c)
    for c in sent_x + sent_c + sent_g:
        c.wait_send()


def writer(a_ref, b_ref, a_out, b_out, sem):
    copies = [pltpu.make_async_copy(a_ref, a_out, sem.at[0]), pltpu.make_async_copy(b_ref, b_out, sem.at[1])]
    for c in copies:
        c.start()
    for c in copies:
        c.wait()


def per_device(x_first, x_second, cotangent, w_attn_in, w_attn_out, w_up, w_down, norm_gains, logit_scales):
    any_spec = pl.BlockSpec(memory_space=pltpu.HBM)
    vmem_spec = pl.BlockSpec(memory_space=pltpu.VMEM)
    tile = (RW, CL, LV, D)
    v = pltpu.VMEM
    scratch = [
        v((3,) + tile, BF), v((2, D, 3 * D), BF), v((2, D, D), BF), v((2, D, FF), BF), v((2, FF, D), BF),
        v((2,) + tile, BF), v((D // 128, NT, 128), F32), v((2, NT, D), F32), v((2, NT, D), F32),
        v((2, NT, D), F32), v((2, NT, 128), F32), v((2, NT, D), F32), v((2, NT, 128), F32),
        v((NT, D), BF), v((2, NT, 2 * D), BF), v((2, NT, D), BF), v((2, NT, 2 * D), F32),
        v((2, 2 * PAIRS, 2 * WT, WT), BF), v((2, 2 * PAIRS, 2 * WT, 128), F32), v((2, NT, D), BF), v((2, NT, FF), F32),
        v((NT, D), F32), v((NT, D), BF), v((NT, FF), BF), v((NT, D), F32), v((NT, D), BF), v((NT, D), BF),
        v((NT, 2 * D), BF), v((NT, 3 * D), BF), v((NT, D), F32), v((2, WT, WT), F32), v((256, 256), BF),
        v(tile, BF), v(tile, BF), v((2, 2, D), F32), pltpu.SMEM((2, HEADS), F32),
        pltpu.SemaphoreType.DMA((7,)), pltpu.SemaphoreType.DMA((8,)),
        pltpu.SemaphoreType.DMA((9,)), pltpu.SemaphoreType.DMA((9,)),
    ]
    body = functools.partial(kernel, lax.axis_size("lat"), lax.axis_size("lon"))
    cells = (1, 2, 0, 3)
    out = pl.pallas_call(
        body,
        out_shape=(jax.ShapeDtypeStruct(tile, F32), jax.ShapeDtypeStruct(tile, F32)),
        in_specs=[any_spec] * 9,
        out_specs=(vmem_spec, vmem_spec),
        scratch_shapes=scratch,
        compiler_params=pltpu.CompilerParams(
            collective_id=0, has_side_effects=True, vmem_limit_bytes=VMEM_LIMIT
        ),
        name="step",
    )(
        *[pltpu.with_memory_space_constraint(v, pltpu.HBM) for v in [jnp.transpose(v, cells) for v in (x_first, x_second, cotangent)] + [
        w_attn_in, w_attn_out, w_up, w_down, norm_gains, logit_scales]],
    )
    out = pl.pallas_call(
        writer,
        out_shape=(jax.ShapeDtypeStruct(tile, F32), jax.ShapeDtypeStruct(tile, F32)),
        in_specs=[vmem_spec, vmem_spec],
        out_specs=(any_spec, any_spec),
        scratch_shapes=[pltpu.SemaphoreType.DMA((2,))],
        compiler_params=pltpu.CompilerParams(vmem_limit_bytes=4 * 1024 * 1024),
        name="write",
    )(*out)
    return tuple(jnp.transpose(v, (2, 0, 1, 3)) for v in out)


def solution(mesh):
    grid = P(None, "lat", "lon", None)
    return jax.shard_map(
        per_device,
        mesh=mesh,
        in_specs=(grid, grid, grid, P(), P(), P(), P(), P(), P()),
        out_specs=(grid, grid),
        check_vma=False,
    )
```

```python
import functools
import math

import jax
import jax.numpy as jnp
from jax import lax
from jax.experimental import pallas as pl
from jax.experimental.pallas import tpu as pltpu
from jax.sharding import PartitionSpec as P

F32 = jnp.float32
BF = jnp.bfloat16
MESH = pl.DeviceIdType.MESH

LV, RW, CL = 4, 6, 12
HR, HC = RW // 2, CL // 2
RC = RW * CL
NT = LV * RW * CL
WT = NT // 2
D, FF, HEADS, HD = 512, 2048, 8, 64
PAIRS = HEADS // 2
EPS = 1e-05
VMEM_LIMIT = 48 * 1024 * 1024
FWD_DEPTH, BWD_DEPTH = 4, 4
QUADS = ((1, 1), (1, 0), (0, 1), (0, 0))
ORDER = ((0, 1, 2, 3), (1, 2, 3, 0))

C0 = math.sqrt(2.0 / math.pi)
C1 = 0.044715


def nn(a, b):
    return lax.dot_general(a, b, (((1,), (0,)), ((), ())), preferred_element_type=F32)


def nt(a, b):
    return lax.dot_general(a, b, (((1,), (1,)), ((), ())), preferred_element_type=F32)


def tn(a, b):
    return lax.dot_general(a, b, (((0,), (0,)), ((), ())), preferred_element_type=F32)


def pipelined(steps, depth):
    waiting, active = list(steps), []
    while waiting or active:
        if waiting and len(active) < depth:
            active.append(waiting.pop(0))
        active = [g for g in active if next(g, active) is not active]


def row_chunks(size=48):
    return [slice(i, i + size) for i in range(0, NT, size)]


def kernel(
    lat_n, lon_n,
    x1_in, x2_in, ct_in, win_in, wout_in, wup_in, wdn_in, gains_in, scales_in,
    g1_out, g2_out,
    tiles, win, wout, wup, wdn,
    moved, flat, xf, dyf, xh1, rstd1, xh2, rstd2, nb, qk, vv, rs, aa, rr, oo, gp,
    rf, dyb, du, dr, drb, dob, dqk, dp, dn, allow, bd,
    gsend, grecv, gains, scales,
    in_sem, w_sem, ssem, rsem,
):
    a = lax.axis_index("lat")
    b = lax.axis_index("lon")
    up, down = lax.rem(a + 1, lat_n), lax.rem(a + lat_n - 1, lat_n)
    east, west = lax.rem(b + 1, lon_n), lax.rem(b + lon_n - 1, lon_n)
    before = ((a, west), (down, b), (down, west))
    after = ((a, east), (up, b), (up, east))

    barrier = pltpu.get_barrier_semaphore()
    for dev in before + after:
        pl.semaphore_signal(barrier, inc=1, device_id=dev, device_id_type=MESH)

    loads = [
        pltpu.make_async_copy(x2_in, tiles.at[0], in_sem.at[0]),
        pltpu.make_async_copy(ct_in, tiles.at[1], in_sem.at[1]),
        pltpu.make_async_copy(x1_in, tiles.at[2], in_sem.at[2]),
        pltpu.make_async_copy(x2_in.at[HR:RW, HC:CL], moved.at[0, 0:HR, 0:HC], in_sem.at[3]),
        pltpu.make_async_copy(ct_in.at[HR:RW, HC:CL], moved.at[1, 0:HR, 0:HC], in_sem.at[4]),
        pltpu.make_async_copy(gains_in, gains, in_sem.at[5]),
        pltpu.make_async_copy(scales_in, scales, in_sem.at[6]),
    ]
    for i in (0, 2, 5, 6, 1, 3, 4):
        loads[i].start()
    weights = {}
    for n, (name, blk) in enumerate(
        (("in", 0), ("out", 0), ("up", 0), ("in", 1), ("out", 1), ("up", 1), ("dn", 1), ("dn", 0))
    ):
        src, dst = {"in": (win_in, win), "out": (wout_in, wout), "up": (wup_in, wup), "dn": (wdn_in, wdn)}[name]
        weights[name, blk] = pltpu.make_async_copy(src.at[blk], dst.at[blk], w_sem.at[n])

    def fetch(*names):
        for n in names:
            weights[n].start()

    fetch(("in", 0))

    def spots(half):
        rq, cq = half
        return [(r, c) for r in range(HR * rq, HR * rq + HR) for c in range(HC * cq, HC * cq + HC)]

    def at(r, c):
        o = LV * (r * CL + c)
        return slice(o, o + LV)

    def levels_apart(dst, order):
        for m, lev in enumerate(order):
            for j in range(D // 128):
                dst[m * RC:m * RC + RC, 128 * j:128 * j + 128] = flat[j, pl.ds(lev, RC, stride=LV), :]

    def levels_together(src, order):
        for m, lev in enumerate(order):
            for j in range(D // 128):
                flat[j, pl.ds(lev, RC, stride=LV), :] = src[m * RC:m * RC + RC, 128 * j:128 * j + 128]

    def set_flat(r, c, v):
        for j in range(D // 128):
            flat[j, at(r, c), :] = v[:, 128 * j:128 * j + 128]

    def get_flat(r, c):
        return jnp.concatenate([flat[j, at(r, c), :] for j in range(D // 128)], axis=1)

    def from_tile(tile, dst, order):
        for r in range(RW):
            for c in range(CL):
                set_flat(r, c, tile[r, c].astype(F32))
        levels_apart(dst, order)

    def block_of(ref, half):
        rq, cq = half
        return ref.at[HR * rq:HR * rq + HR, HC * cq:HC * cq + HC]

    def swapped(half):
        return (1 - half[0], 1 - half[1])

    def send(src, dst, half, dev, n):
        c = pltpu.make_async_remote_copy(
            src_ref=block_of(src, half), dst_ref=block_of(dst, swapped(half)),
            send_sem=ssem.at[n], recv_sem=rsem.at[n], device_id=dev, device_id_type=MESH,
        )
        c.start()
        return c

    loads[0].wait()
    pl.semaphore_wait(barrier, 6)
    sent_x = [send(tiles.at[0], moved.at[0], QUADS[q], before[q - 1], q - 1) for q in (3, 2, 1)]
    sent_c = []

    def send_cotangent():
        loads[1].wait()
        sent_c.extend(send(tiles.at[1], moved.at[1], QUADS[q], before[q - 1], q + 2) for q in (3, 2, 1))

    loads[2].wait()
    fetch(("out", 0), ("up", 0))
    from_tile(tiles.at[2], xf.at[0], ORDER[0])
    loads[5].wait()
    loads[6].wait()

    ri = lax.broadcasted_iota(jnp.int32, (256, 256), 0)
    ci = lax.broadcasted_iota(jnp.int32, (256, 256), 1)
    bd[...] = (lax.shift_right_logical(ri, 6) == lax.shift_right_logical(ci, 6)).astype(F32).astype(BF)
    last_band = (a == lat_n - 1).astype(jnp.int32)
    for w in range(2):
        labels = []
        for axis in (0, 1):
            t = lax.broadcasted_iota(jnp.int32, (WT, WT), axis)
            second = (t >= RC).astype(jnp.int32)
            late_rows = (t - RC * second >= RC // 2).astype(jnp.int32)
            lab = 2 * last_band * late_rows
            if w == 1:
                lab = lab + second
            labels.append(lab)
        allow[w] = (labels[0] == labels[1]).astype(F32)
    lane = lax.broadcasted_iota(jnp.int32, (WT, 128), 1)
    first_half = lane < HD
    m_a = first_half.astype(F32).astype(BF)
    m_b = (lane >= HD).astype(F32).astype(BF)
    ones = jnp.ones((WT, 128), BF)

    def stacked(v):
        return jnp.concatenate([v * m_a, v * m_b], axis=0)

    def wide(r):
        return jnp.concatenate([r, r[:, :WT - 128]], axis=1)

    def layer_norm(src, gain, xh, rstd):
        for s in row_chunks():
            x = src[s, :]
            c = x - jnp.mean(x, axis=-1, keepdims=True)
            inv = lax.rsqrt(jnp.mean(c * c, axis=-1, keepdims=True) + EPS)
            h = c * inv
            xh[s, :] = h
            rstd[s, :] = jnp.broadcast_to(inv, (h.shape[0], 128))
            nb[s, :] = (h * gain).astype(BF)

    def layer_norm_back(base, grad, gain, xh, rstd, dst, dst_bf=None):
        for s in row_chunks():
            g = grad[s, :] * gain
            h = xh[s, :]
            m1 = jnp.mean(g, axis=-1, keepdims=True)
            m2 = jnp.mean(g * h, axis=-1, keepdims=True)
            inv = rstd[s, 0:1]
            v = base[s, :] + inv * (g - m1 - h * m2)
            dst[s, :] = v
            if dst_bf is not None:
                dst_bf[s, :] = v.astype(BF)

    def forward(k):
        x = xf.at[k]
        layer_norm(x, gains[k, 0:1, :], xh1.at[k], rstd1.at[k])
        weights["in", k].wait()
        if k == 0:
            fetch(("in", 1), ("out", 1), ("up", 1))
        n1 = nb[...]
        for j in range(6):
            c = slice(256 * j, 256 * j + 256)
            p = nn(n1, win[k, :, c])
            if j < 4:
                inv = lax.rsqrt(nn((p * p).astype(BF), bd[...]) + 1e-06)
                rs[k, :, c] = inv
                qk[k, :, c] = (p * inv).astype(BF)
            else:
                vv[k, :, 256 * (j - 4):256 * (j - 4) + 256] = p.astype(BF)
        def attend(w, pr):
            rows = slice(WT * w, WT * w + WT)
            it = w * PAIRS + pr
            c = slice(128 * pr, 128 * pr + 128)
            ck = slice(D + 128 * pr, D + 128 * pr + 128)
            s = nt(stacked(qk[k, rows, c]), qk[k, rows, ck])
            yield
            ea = jnp.exp(s[:WT] * scales[k, 2 * pr])
            eb = jnp.exp(s[WT:] * scales[k, 2 * pr + 1])
            if k == 1:
                ea = ea * allow[w]
                eb = eb * allow[w]
            e = jnp.concatenate([ea, eb], axis=0).astype(BF)
            aa[k, it] = e
            yield
            ou = nn(e, jnp.concatenate([vv[k, rows, c], ones], axis=1))
            yield
            r = 1.0 / ou[:, 128:]
            rr[k, it] = r
            on = ou[:, :128] * r
            oo[k, rows, c] = jnp.where(first_half, on[:WT], on[WT:]).astype(BF)

        pipelined([attend(w, pr) for pr in range(PAIRS) for w in range(2)], FWD_DEPTH)
        if k == 0:
            send_cotangent()
        weights["out", k].wait()
        o = oo[k]
        for j in range(2):
            c = slice(256 * j, 256 * j + 256)
            rf[:, c] = x[:, c] + nn(o, wout[k, :, c])
        layer_norm(rf, gains[k, 1:2, :], xh2.at[k], rstd2.at[k])
        weights["up", k].wait()
        if k == 0:
            fetch(("dn", 1), ("dn", 0))
        n2 = nb[...]
        for j in range(8):
            c = slice(256 * j, 256 * j + 256)
            u = nn(n2, wup[k, :, c]).astype(BF)
            u2 = u * u
            t = jnp.tanh(u * (C0 + (C0 * C1) * u2))
            gp[k, :, c] = (0.5 + 0.5 * t) + (1.0 - t * t) * (u * (0.5 * C0 + (1.5 * C0 * C1) * u2))

    def backward(k):
        dy = dyf.at[k]
        for s in row_chunks():
            dyb[s, :] = dy[s, :].astype(BF)
        weights["dn", k].wait()
        g = dyb[...]
        for j in range(8):
            c = slice(256 * j, 256 * j + 256)
            du[:, c] = nt(g, wdn[k, c, :]).astype(BF) * gp[k, :, c]
        g = du[...]
        for j in range(2):
            c = slice(256 * j, 256 * j + 256)
            dn[:, c] = nt(g, wup[k, c, :])
        layer_norm_back(dy, dn, gains[k, 1:2, :], xh2.at[k], rstd2.at[k], dr, drb)
        g = drb[...]
        for j in range(2):
            c = slice(256 * j, 256 * j + 256)
            dob[:, c] = nt(g, wout[k, c, :]).astype(BF)
        def attend_back(w, pr):
            rows = slice(WT * w, WT * w + WT)
            it = w * PAIRS + pr
            c = slice(128 * pr, 128 * pr + 128)
            ck = slice(D + 128 * pr, D + 128 * pr + 128)
            do = dob[rows, c]
            dos = stacked(do)
            dpr = nt(dos, vv[k, rows, c])
            prod = do.astype(F32) * oo[k, rows, c].astype(F32)
            da = jnp.sum(jnp.where(first_half, prod, 0.0), axis=-1, keepdims=True)
            db = jnp.sum(jnp.where(first_half, 0.0, prod), axis=-1, keepdims=True)
            e = aa[k, it]
            r = rr[k, it]
            dor = (dos.astype(F32) * r).astype(BF)
            dp[rows, 2 * D + 128 * pr:2 * D + 128 * pr + 128] = tn(e, dor).astype(BF)
            yield
            ra = wide(r[:WT] * scales[k, 2 * pr])
            rb = wide(r[WT:] * scales[k, 2 * pr + 1])
            e32 = e.astype(F32)
            dsa = e32[:WT] * ra * (dpr[:WT] - da)
            dsb = e32[WT:] * rb * (dpr[WT:] - db)
            ds = jnp.concatenate([dsa, dsb], axis=0).astype(BF)
            yield
            dq = nn(ds, qk[k, rows, ck])
            dqk[rows, ck] = tn(ds, stacked(qk[k, rows, c])).astype(BF)
            yield
            dqk[rows, c] = jnp.where(first_half, dq[:WT], dq[WT:]).astype(BF)

        pipelined([attend_back(w, pr) for pr in range(PAIRS) for w in range(2)], BWD_DEPTH)
        for j in range(4):
            c = slice(256 * j, 256 * j + 256)
            g = dqk[:, c].astype(F32)
            h = qk[k, :, c].astype(F32)
            dot = nn((g * h).astype(BF), bd[...])
            dp[:, c] = (rs[k, :, c] * (g - h * dot)).astype(BF)
        g = dp[...]
        for j in range(2):
            c = slice(256 * j, 256 * j + 256)
            dn[:, c] = nt(g, win[k, c, :])
        layer_norm_back(dr, dn, gains[k, 0:1, :], xh1.at[k], rstd1.at[k], rf)

    forward(0)

    loads[3].wait()
    for c in sent_x:
        c.wait_recv()
    from_tile(moved.at[0], xf.at[1], ORDER[1])
    forward(1)
    loads[4].wait()
    for c in sent_c:
        c.wait_recv()
    from_tile(moved.at[1], dyf.at[1], ORDER[1])
    backward(1)

    levels_together(rf, ORDER[1])
    sent_g = []
    for q in (3, 2, 1):
        for r, c in spots(swapped(QUADS[q])):
            gsend[r, c] = get_flat(r, c).astype(BF)
    for q in (3, 2, 1):
        sent_g.append(send(gsend, grecv, swapped(QUADS[q]), after[q - 1], q + 5))
    own = {(r + HR, c + HC): get_flat(r, c) for r, c in spots((0, 0))}
    for (r, c), v in own.items():
        set_flat(r, c, v)
        g2_out[r, c] = v
    for q in (1, 2, 3):
        sent_g[3 - q].wait_recv()
        for r, c in spots(QUADS[q]):
            v = grecv[r, c].astype(F32)
            set_flat(r, c, v)
            g2_out[r, c] = v
    levels_apart(dyf.at[0], ORDER[0])
    backward(0)
    levels_together(rf, ORDER[0])
    for r in range(RW):
        for c in range(CL):
            g1_out[r, c] = get_flat(r, c)
    for c in sent_x + sent_c + sent_g:
        c.wait_send()


def writer(a_ref, b_ref, a_out, b_out, sem):
    copies = [pltpu.make_async_copy(a_ref, a_out, sem.at[0]), pltpu.make_async_copy(b_ref, b_out, sem.at[1])]
    for c in copies:
        c.start()
    for c in copies:
        c.wait()


def per_device(x_first, x_second, cotangent, w_attn_in, w_attn_out, w_up, w_down, norm_gains, logit_scales):
    any_spec = pl.BlockSpec(memory_space=pltpu.HBM)
    vmem_spec = pl.BlockSpec(memory_space=pltpu.VMEM)
    tile = (RW, CL, LV, D)
    v = pltpu.VMEM
    scratch = [
        v((3,) + tile, BF), v((2, D, 3 * D), BF), v((2, D, D), BF), v((2, D, FF), BF), v((2, FF, D), BF),
        v((2,) + tile, BF), v((D // 128, NT, 128), F32), v((2, NT, D), F32), v((2, NT, D), F32),
        v((2, NT, D), F32), v((2, NT, 128), F32), v((2, NT, D), F32), v((2, NT, 128), F32),
        v((NT, D), BF), v((2, NT, 2 * D), BF), v((2, NT, D), BF), v((2, NT, 2 * D), F32),
        v((2, 2 * PAIRS, 2 * WT, WT), BF), v((2, 2 * PAIRS, 2 * WT, 128), F32), v((2, NT, D), BF), v((2, NT, FF), BF),
        v((NT, D), F32), v((NT, D), BF), v((NT, FF), BF), v((NT, D), F32), v((NT, D), BF), v((NT, D), BF),
        v((NT, 2 * D), BF), v((NT, 3 * D), BF), v((NT, D), F32), v((2, WT, WT), F32), v((256, 256), BF),
        v(tile, BF), v(tile, BF), v((2, 2, D), F32), pltpu.SMEM((2, HEADS), F32),
        pltpu.SemaphoreType.DMA((7,)), pltpu.SemaphoreType.DMA((8,)),
        pltpu.SemaphoreType.DMA((9,)), pltpu.SemaphoreType.DMA((9,)),
    ]
    body = functools.partial(kernel, lax.axis_size("lat"), lax.axis_size("lon"))
    cells = (1, 2, 0, 3)
    out = pl.pallas_call(
        body,
        out_shape=(jax.ShapeDtypeStruct(tile, F32), jax.ShapeDtypeStruct(tile, F32)),
        in_specs=[any_spec] * 9,
        out_specs=(vmem_spec, vmem_spec),
        scratch_shapes=scratch,
        compiler_params=pltpu.CompilerParams(
            collective_id=0, has_side_effects=True, vmem_limit_bytes=VMEM_LIMIT
        ),
        name="step",
    )(
        *[pltpu.with_memory_space_constraint(v, pltpu.HBM) for v in [jnp.transpose(v, cells) for v in (x_first, x_second, cotangent)] + [
        w_attn_in, w_attn_out, w_up, w_down, norm_gains, logit_scales]],
    )
    out = pl.pallas_call(
        writer,
        out_shape=(jax.ShapeDtypeStruct(tile, F32), jax.ShapeDtypeStruct(tile, F32)),
        in_specs=[vmem_spec, vmem_spec],
        out_specs=(any_spec, any_spec),
        scratch_shapes=[pltpu.SemaphoreType.DMA((2,))],
        compiler_params=pltpu.CompilerParams(vmem_limit_bytes=4 * 1024 * 1024),
        name="write",
    )(*out)
    return tuple(jnp.transpose(v, (2, 0, 1, 3)) for v in out)


def solution(mesh):
    grid = P(None, "lat", "lon", None)
    return jax.shard_map(
        per_device,
        mesh=mesh,
        in_specs=(grid, grid, grid, P(), P(), P(), P(), P(), P()),
        out_specs=(grid, grid),
        check_vma=False,
    )
```
